256 devices in a mesh: mkt: 8 (over x, core), trade: 8 (over y, z_hi), scen: 4 (over z_lo).
Axes of the slice: x: 4, y: 4, z: 8 (z_hi: 2, z_lo: 4; z = z_hi * 4 + z_lo), core: 2. Of those that a mesh axis runs over, the one named last changes fastest.
Arguments:
- quotes: bfloat16 [512, 4096], P('mkt'), may hold values from -6 to 6
- kernel: bfloat16 [512, 128, 128], P(('trade', 'scen')), may hold values from -0.5 to 0.5
- trade_block: int32 [16384], P('trade'), may hold values from 0 to 511
- trade_embed: bfloat16 [16384, 256], P('trade'), may hold values from -6 to 6
- position: float32 [16384], P('trade'), may hold values from -0.046875 to 0.046875
- scen_rank: int32 [512], P(('mkt', 'scen')), may hold values from 0 to 511, each once
- w_in: bfloat16 [128, 256], replicated, may hold values from -0.5 to 0.5
- w_mid: bfloat16 [256, 256], replicated, may hold values from -0.375 to 0.375
- b_mid: float32 [256], replicated, may hold values from -6 to 6
- w_out: bfloat16 [256], replicated, may hold values from -0.375 to 0.375
Outputs:
- book_pnl: float32 [512], P(('mkt', 'scen'))
- marginal: float32 [16384], P('trade')
- shortfall: float32 [], replicated
The draws below stay inside these ranges and needn't reach their ends.
Inputs may be any that keep to these rules, and one draw needn't show every extreme that they name: scen_rank holds each rank of 0 to 511 once.
All inputs are finite; a program needn't handle non-finite values.
Results may differ from the reference program's by a relative error of at most 0.014.
The reference program's roundings to bfloat16 on the way count: a program that leaves them out, or rounds other values in their place, can miss the bound.
Values may be sent and summed in bfloat16 or wider, within the bound.
A program may use at most 64 MiB of HBM per device.

```python
import jax
import jax.numpy as jnp
from jax import lax

SEG = 128
WIN = 128
QSTEP = 8
HID = 256
NB = 512
Q = 4096
S = 512
TRADES = 16384
RSPAN = 25


def with_ends(values, stream_key, low, high):
    extent = values.shape
    place = [jax.random.randint(jax.random.fold_in(stream_key, axis), (), 0, extent[axis]) for axis in range(len(extent))]
    values = values.at[tuple(place)].set(low)
    longest = extent.index(max(extent))
    place[longest] = (place[longest] + 1) % extent[longest]
    return values.at[tuple(place)].set(high)


def shard_levels(key, extent, cuts, smallest, high):
    level, own = 1.0, jax.random.fold_in(key, 6)
    for dim, blocks in cuts:
        draws = jnp.exp(jax.random.uniform(jax.random.fold_in(own, dim), (blocks,), jnp.float32, smallest / len(cuts), high / len(cuts)))
        level = level * jnp.repeat(draws, extent[dim] // blocks).reshape([-1 if axis == dim else 1 for axis in range(len(extent))])
    return level


def bell_draw(key, dims, width, limit, shards=(), held_as=jnp.bfloat16):
    level = shard_levels(key, dims, shards, -0.22, 0.18) if shards else 1.0
    drawn = jax.random.normal(key, dims, jnp.float32) * width * level
    return jnp.minimum(jnp.maximum(drawn, -limit), limit).astype(held_as)


def setup_inputs(seed: int = 0) -> dict:
    streams_of = jax.random.split(jax.random.key(seed), 11)
    return {
        "quotes": bell_draw(streams_of[0], (S, Q), 1.0, 6.0, ((0, 8),)),
        "kernel": bell_draw(streams_of[1], (NB, WIN, SEG), WIN ** -0.5, 0.5, ((0, 32),)),
        "trade_block": with_ends(jax.random.randint(streams_of[2], (TRADES,), 0, NB), jax.random.fold_in(streams_of[2], 1), 0, NB - 1).astype(jnp.int32),
        "trade_embed": bell_draw(streams_of[3], (TRADES, HID), 1.0, 6.0, ((0, 8),)),
        "position": bell_draw(streams_of[4], (TRADES,), TRADES ** -0.5, 0.046875, ((0, 8),), jnp.float32),
        "scen_rank": jax.random.permutation(streams_of[5], S).astype(jnp.int32),
        "w_in": bell_draw(streams_of[6], (SEG, HID), SEG ** -0.5, 0.5),
        "w_mid": bell_draw(streams_of[7], (HID, HID), HID ** -0.5, 0.375),
        "b_mid": bell_draw(streams_of[8], (HID,), 1.0, 6.0, (), jnp.float32),
        "w_out": bell_draw(streams_of[9], (HID,), HID ** -0.5, 0.375),
    }


def reference(quotes, kernel, trade_block, trade_embed, position, scen_rank, w_in, w_mid, b_mid, w_out):
    def build(block_pair):
        block_index, block_kernel = block_pair
        window_start = jnp.clip(QSTEP * block_index - (WIN - QSTEP) // 2, 0, Q - WIN).astype(jnp.int32)
        window = lax.dynamic_slice_in_dim(quotes, window_start, WIN, 1)
        return jnp.dot(window, block_kernel, preferred_element_type=jnp.float32).astype(jnp.bfloat16)

    states = lax.map(build, (jnp.arange(NB, dtype=jnp.int32), kernel))

    def price(scen_index):
        curve_table = lax.dynamic_index_in_dim(states, scen_index, 1, keepdims=False)
        trade_rows = curve_table[trade_block]
        hidden_one = jax.nn.silu(jnp.dot(trade_rows, w_in, preferred_element_type=jnp.float32) + trade_embed.astype(jnp.float32)).astype(jnp.bfloat16)
        hidden_two = jax.nn.silu(jnp.dot(hidden_one, w_mid, preferred_element_type=jnp.float32) + b_mid).astype(jnp.bfloat16)
        return jnp.dot(hidden_two, w_out, preferred_element_type=jnp.float32)

    values = lax.map(price, jnp.arange(S, dtype=jnp.int32))
    book_pnl = jnp.dot(values, position, precision=lax.Precision.HIGHEST)
    weight_sum = jnp.sum(jnp.exp(-jnp.arange(S, dtype=jnp.float32) / RSPAN))
    weights = jnp.exp(-scen_rank.astype(jnp.float32) / RSPAN) / weight_sum
    marginal = -jnp.dot(weights, values, precision=lax.Precision.HIGHEST)
    shortfall = -jnp.dot(weights, book_pnl, precision=lax.Precision.HIGHEST)
    return book_pnl, marginal, shortfall
```

```python
import functools
import math

import jax
import jax.numpy as jnp
from jax import lax
from jax.experimental import pallas as pl
from jax.experimental.pallas import tpu as pltpu
from jax.sharding import PartitionSpec as P

SEG = 128
WIN = 128
QSTEP = 8
HIGHEST = lax.Precision.HIGHEST
UNROLL = 4


def copy_for_each(x, axis):
    size = lax.axis_size(axis)
    return lax.all_to_all(jnp.broadcast_to(x[None], (size, *x.shape)), axis, 0, 0, tiled=True)


def of_everyone(x, axis):
    return copy_for_each(x, axis).sum(axis=0)


def prepare(w_in, w_mid, b_mid, w_out, embed, e32, w1, w2t, b2, w3):
    w1[...] = (w_in[...].astype(jnp.float32) * 0.5).astype(jnp.bfloat16)
    w2t[...] = (w_mid[...].astype(jnp.float32).T * 0.5).astype(jnp.bfloat16)
    b2[...] = jnp.broadcast_to(b_mid[...].reshape(1, -1) * 0.5, b2.shape[::-1]).T
    w3[...] = jnp.broadcast_to(w_out[...].reshape(1, -1), w3.shape)

    @pl.loop(0, embed.shape[0] // 64)
    def _(i):
        r = pl.multiple_of(i * 64, 64)
        t = embed[pl.ds(r, 64), :].astype(jnp.float32) * 0.5
        e32[0, pl.ds(r, 64), :] = t[:, :128]
        e32[1, pl.ds(r, 64), :] = t[:, 128:]


def price(idx, table, e32, w1, w2t, b2, w3, h1, h2, values):
    groups = values.shape[0]
    u_count = UNROLL

    def first(g, slot):
        x = jnp.concatenate([table[idx[j * groups + g]] for j in range(16)], axis=0)
        e = jnp.concatenate(
            [
                jnp.concatenate([e32.at[h][pl.ds(j * groups + g, 16, stride=0), :] for j in range(16)], axis=0)
                for h in range(2)
            ],
            axis=1,
        )
        z = jnp.dot(x, w1[...], preferred_element_type=jnp.float32) + e
        h1[slot] = (z + z * jnp.tanh(z)).astype(jnp.bfloat16)

    def second(slot):
        z = lax.dot_general(w2t[...], h1[slot], (((1,), (1,)), ((), ())), preferred_element_type=jnp.float32)
        z = z + b2[...]
        h2[slot] = (z + z * jnp.tanh(z)).astype(jnp.bfloat16)

    def third(g, slot):
        v = jnp.dot(w3[...], h2[slot], preferred_element_type=jnp.float32)
        values[pl.ds(g, 1), :] = v[0:1, :]

    def half(i, a, b):
        for u in range(u_count):
            first(jnp.minimum((i + 2) * u_count + u, groups - 1), a + u)
            second(b + u)
            third(i * u_count + u, a + u)

    for u in range(u_count):
        first(u, u)
    for u in range(u_count):
        second(u)
        first(u_count + u, u_count + u)

    @pl.loop(0, groups // u_count // 2)
    def _(k):
        half(2 * k, 0, u_count)
        half(2 * k + 1, u_count, 0)


def reduce_values(rank, position, values, span, weight_sum, marg, pnl):
    groups, width = values.shape
    row = lax.broadcasted_iota(jnp.int32, (16, width), 0)
    lane = lax.broadcasted_iota(jnp.int32, (16, width), 1)
    ranks = jnp.zeros((16, width), jnp.float32)
    for s in range(16):
        ranks = jnp.where(lane % 16 == s, rank[s].astype(jnp.float32), ranks)
    weights = jnp.exp(-ranks / span) * (1.0 / weight_sum)
    mine = row == lane // 16
    v = values[...]
    marg[...] = -lax.dot_general(
        jnp.where(mine, weights, 0.0), v, (((1,), (1,)), ((), ())),
        precision=HIGHEST, preferred_element_type=jnp.float32,
    )
    spread = jnp.dot(
        position[...].T, jnp.where(mine, 1.0, 0.0), precision=HIGHEST, preferred_element_type=jnp.float32
    )
    held = jnp.sum(v * spread, axis=0, keepdims=True)
    fold = (
        lax.broadcasted_iota(jnp.int32, (width, 128), 0) % 16 == lax.broadcasted_iota(jnp.int32, (width, 128), 1)
    )
    pnl[...] = jnp.dot(
        jnp.broadcast_to(held, (8, width)), jnp.where(fold, 1.0, 0.0),
        precision=HIGHEST, preferred_element_type=jnp.float32,
    )


def pricing_kernel(
    span, weight_sum, idx, rank, table, embed, position, w_in, w_mid, b_mid, w_out, marg, pnl,
    e32, w1, w2t, b2, w3, h1, h2, values,
):
    prepare(w_in, w_mid, b_mid, w_out, embed, e32, w1, w2t, b2, w3)
    price(idx, table, e32, w1, w2t, b2, w3, h1, h2, values)
    reduce_values(rank, position, values, span, weight_sum, marg, pnl)


def local(quotes, kernel, trade_block, trade_embed, position, scen_rank, w_in, w_mid, b_mid, w_out):
    local_count = kernel.shape[0]
    rows, quote_count = quotes.shape
    part = lax.axis_index(("trade", "scen"))
    block = part * local_count + jnp.arange(local_count, dtype=jnp.int32)
    start = jnp.clip(QSTEP * block - (WIN - QSTEP) // 2, 0, quote_count - WIN)
    base = jnp.clip((part - 1) * 128, 0, quote_count - 384)
    slab = lax.dynamic_slice_in_dim(quotes, base, 384, 1)
    pick = (
        jnp.arange(384, dtype=jnp.int32)[:, None]
        == ((start - base)[:, None] + jnp.arange(WIN, dtype=jnp.int32)[None, :]).reshape(1, -1)
    )
    windows = jnp.dot(slab, pick.astype(jnp.bfloat16), preferred_element_type=jnp.float32).astype(jnp.bfloat16)
    windows = windows.reshape(rows, local_count, WIN).transpose(1, 0, 2)
    built = jnp.einsum("jrw,jws->jrs", windows, kernel, preferred_element_type=jnp.float32)
    built = built.astype(jnp.bfloat16).reshape(local_count, rows * SEG)
    quarter = lax.all_to_all(built, "scen", split_axis=1, concat_axis=0, tiled=True)
    table = copy_for_each(quarter, "trade").reshape(-1, 16, SEG)

    scen_total = scen_rank.shape[0] * lax.axis_size("mkt") * lax.axis_size("scen")
    span = scen_total // 20
    weight_sum = math.fsum(math.exp(-r / span) for r in range(scen_total))
    trades, hid = trade_embed.shape
    groups = trades // 16
    slots = 2 * UNROLL
    vmem, smem = pl.BlockSpec(memory_space=pltpu.VMEM), pl.BlockSpec(memory_space=pltpu.SMEM)
    marg, pnl = pl.pallas_call(
        functools.partial(pricing_kernel, span, weight_sum),
        out_shape=(
            jax.ShapeDtypeStruct((16, groups), jnp.float32),
            jax.ShapeDtypeStruct((8, 128), jnp.float32),
        ),
        in_specs=[smem, smem] + [vmem] * 7,
        out_specs=(vmem, vmem),
        scratch_shapes=[
            pltpu.VMEM((2, trades, 128), jnp.float32),
            pltpu.VMEM((SEG, hid), jnp.bfloat16),
            pltpu.VMEM((hid, hid), jnp.bfloat16),
            pltpu.VMEM((hid, 256), jnp.float32),
            pltpu.VMEM((16, hid), jnp.bfloat16),
            pltpu.VMEM((slots, 256, hid), jnp.bfloat16),
            pltpu.VMEM((slots, hid, 256), jnp.bfloat16),
            pltpu.VMEM((groups, 256), jnp.float32),
        ],
        compiler_params=pltpu.CompilerParams(vmem_limit_bytes=48 << 20),
        name="price",
    )(trade_block, scen_rank, table, trade_embed, position.reshape(16, groups), w_in, w_mid, b_mid, w_out)

    marginal = of_everyone(marg, ("mkt", "scen"))
    own_share = jnp.sum(position * marginal.reshape(-1))
    both = of_everyone(jnp.concatenate([pnl[0, :16], own_share[None]]), "trade")
    return (both[:16], marginal.reshape(-1), both[16])


def solution(mesh):
    placed = (
        P("mkt", None),
        P(("trade", "scen"), None, None),
        P("trade"),
        P("trade", None),
        P("trade"),
        P(("mkt", "scen")),
        P(),
        P(),
        P(),
        P(),
    )
    return jax.shard_map(
        local,
        mesh=mesh,
        in_specs=placed,
        out_specs=(P(("mkt", "scen")), P("trade"), P()),
        check_vma=False,
    )
```

```python
import functools
import math

import jax
import jax.numpy as jnp
from jax import lax
from jax.experimental import pallas as pl
from jax.experimental.pallas import tpu as pltpu
from jax.sharding import PartitionSpec as P

SEG = 128
WIN = 128
QSTEP = 8
SLAB = 384
HIGHEST = lax.Precision.HIGHEST
MESH = pl.DeviceIdType.MESH
UNROLL = 4


def prepare(w_in, w_mid, b_mid, w_out, embed, e32, w1, w2t, b2, w3):
    w1[...] = (w_in[...].astype(jnp.float32) * 0.5).astype(jnp.bfloat16)
    w2t[...] = (w_mid[...].astype(jnp.float32).T * 0.5).astype(jnp.bfloat16)
    b2[...] = jnp.broadcast_to(b_mid[...].reshape(1, -1) * 0.5, b2.shape[::-1]).T
    w3[...] = jnp.broadcast_to(w_out[...].reshape(1, -1), w3.shape)

    @pl.loop(0, embed.shape[0] // 64)
    def _(i):
        r = pl.multiple_of(i * 64, 64)
        t = embed[pl.ds(r, 64), :].astype(jnp.float32) * 0.5
        e32[0, pl.ds(r, 64), :] = t[:, :128]
        e32[1, pl.ds(r, 64), :] = t[:, 128:]


def price(idx, table, e32, w1, w2t, b2, w3, h1, h2, values):
    groups = values.shape[0]
    u_count = UNROLL

    def first(g, slot):
        x = jnp.concatenate([table[idx[j * groups + g]] for j in range(16)], axis=0)
        e = jnp.concatenate(
            [
                jnp.concatenate([e32.at[h][pl.ds(j * groups + g, 16, stride=0), :] for j in range(16)], axis=0)
                for h in range(2)
            ],
            axis=1,
        )
        z = jnp.dot(x, w1[...], preferred_element_type=jnp.float32) + e
        h1[slot] = (z + z * jnp.tanh(z)).astype(jnp.bfloat16)

    def second(slot):
        z = lax.dot_general(w2t[...], h1[slot], (((1,), (1,)), ((), ())), preferred_element_type=jnp.float32)
        z = z + b2[...]
        h2[slot] = (z + z * jnp.tanh(z)).astype(jnp.bfloat16)

    def third(g, slot):
        v = jnp.dot(w3[...], h2[slot], preferred_element_type=jnp.float32)
        values[pl.ds(g, 1), :] = v[0:1, :]

    def half(i, a, b):
        for u in range(u_count):
            first(jnp.minimum((i + 2) * u_count + u, groups - 1), a + u)
            second(b + u)
            third(i * u_count + u, a + u)

    for u in range(u_count):
        first(u, u)
    for u in range(u_count):
        second(u)
        first(u_count + u, u_count + u)

    @pl.loop(0, groups // u_count // 2)
    def _(k):
        half(2 * k, 0, u_count)
        half(2 * k + 1, u_count, 0)


def reduce_values(rank, position, values, span, weight_sum, marg, pnl):
    groups, width = values.shape
    row = lax.broadcasted_iota(jnp.int32, (16, width), 0)
    lane = lax.broadcasted_iota(jnp.int32, (16, width), 1)
    ranks = jnp.zeros((16, width), jnp.float32)
    for s in range(16):
        ranks = jnp.where(lane % 16 == s, rank[s].astype(jnp.float32), ranks)
    weights = jnp.exp(-ranks / span) * (1.0 / weight_sum)
    mine = row == lane // 16
    v = values[...]
    marg[0:16] = -lax.dot_general(
        jnp.where(mine, weights, 0.0), v, (((1,), (1,)), ((), ())),
        precision=HIGHEST, preferred_element_type=jnp.float32,
    )
    spread = jnp.dot(
        position[...].T, jnp.where(mine, 1.0, 0.0), precision=HIGHEST, preferred_element_type=jnp.float32
    )
    held = jnp.sum(v * spread, axis=0, keepdims=True)
    marg[16:24] = jnp.broadcast_to(-jnp.sum(held * weights[0:1], axis=1, keepdims=True), (8, groups))
    fold = (
        lax.broadcasted_iota(jnp.int32, (width, 128), 0) % 16 == lax.broadcasted_iota(jnp.int32, (width, 128), 1)
    )
    pnl[...] = jnp.dot(
        jnp.broadcast_to(held, (8, width)), jnp.where(fold, 1.0, 0.0),
        precision=HIGHEST, preferred_element_type=jnp.float32,
    )


def build(slab, kernel, offset, built, table, part, scen):
    rows = slab.shape[0]
    for j in range(kernel.shape[0]):
        pick = lax.broadcasted_iota(jnp.int32, (SLAB, WIN), 0) == lax.broadcasted_iota(jnp.int32, (SLAB, WIN), 1) + offset(j)
        window = jnp.dot(
            slab[...], jnp.where(pick, 1.0, 0.0).astype(jnp.bfloat16), preferred_element_type=jnp.float32
        ).astype(jnp.bfloat16)
        state = jnp.dot(window, kernel[j], preferred_element_type=jnp.float32).astype(jnp.bfloat16)
        for q in range(rows // 16):
            built[q, j] = state[16 * q : 16 * q + 16]


def fused_kernel(
    span, weight_sum, quote_count,
    quotes_hbm, kernel_hbm, embed_hbm, idx, rank, position, w_in, w_mid, b_mid, w_out,
    marg_out, pnl_out, short_out,
    slab, kernel, embed, built, table, e32, w1, w2t, b2, w3, h1, h2, values, msg, pnl,
    got_mkt, got_pnl, got_marg, got_short, load_sem, z_send, y_send, recv, t_send, r_mkt, r_pnl, r_marg, r_short,
):
    mkt, trade, scen = lax.axis_index("mkt"), lax.axis_index("trade"), lax.axis_index("scen")
    y, z_hi = trade // 2, trade % 2
    z = z_hi * 4 + scen
    part = y * 8 + z
    blocks = kernel.shape[0]

    def at_z(zz):
        return {"trade": y * 2 + zz // 4, "scen": zz % 4}

    def at_y(yy):
        return {"trade": yy * 2 + z_hi}

    base = jnp.clip((part - 1) * 128, 0, quote_count - SLAB)
    loads = [
        pltpu.make_async_copy(quotes_hbm.at[:, pl.ds(pl.multiple_of(base, 128), SLAB)], slab, load_sem.at[0]),
        pltpu.make_async_copy(kernel_hbm, kernel, load_sem.at[1]),
        pltpu.make_async_copy(embed_hbm, embed, load_sem.at[2]),
    ]
    for load in loads:
        load.start()

    barrier = pltpu.get_barrier_semaphore()
    for k in range(1, 8):
        pl.semaphore_signal(barrier, inc=1, device_id={"mkt": (mkt + k) % 8}, device_id_type=MESH)
    for k in range(1, 32):
        other = (part + k) % 32
        pl.semaphore_signal(
            barrier, inc=1, device_id={"trade": other // 4, "scen": other % 4}, device_id_type=MESH
        )

    def offset(j):
        return jnp.clip(QSTEP * (part * blocks + j) - (WIN - QSTEP) // 2, 0, quote_count - WIN) - base

    loads[0].wait()
    loads[1].wait()
    build(slab, kernel, offset, built, table, part, scen)
    table[pl.ds(part * blocks, blocks)] = built[scen]
    pl.semaphore_wait(barrier, 38)

    def piece(p):
        return table.at[pl.ds(p * blocks, blocks)]

    def copy(src, dst, send, receive, device):
        return pltpu.make_async_remote_copy(
            src_ref=src, dst_ref=dst, send_sem=send, recv_sem=receive, device_id=device, device_id_type=MESH
        )

    sends = []

    def send(*args):
        c = copy(*args)
        c.start()
        sends.append(c)

    def await_piece(p):
        copy(piece(p), piece(p), y_send.at[0], recv.at[p], at_y((y + 1) % 4)).wait_recv()

    steps = (1, 7, 2, 6, 3, 5, 4)
    for k, d in enumerate(steps):
        to = (z + d) % 8
        send(built.at[to % 4], piece(part), z_send.at[k], recv.at[part], at_z(to))
    up, down = (y + 1) % 4, (y + 3) % 4
    arrivals = (0,) + tuple(8 - d for d in steps)
    for k, d in enumerate(arrivals):
        source = (z + d) % 8
        p = y * 8 + source
        if d:
            await_piece(p)
        send(piece(p), piece(p), y_send.at[3 * k], recv.at[p], at_y(up))
        send(piece(p), piece(p), y_send.at[3 * k + 1], recv.at[p], at_y(down))
        if k == 0:
            loads[2].wait()
            prepare(w_in, w_mid, b_mid, w_out, embed, e32, w1, w2t, b2, w3)
        even = source % 2 == 0
        near, far = jnp.where(even, down, up), jnp.where(even, up, down)
        p = near * 8 + source
        await_piece(p)
        send(piece(p), piece(p), y_send.at[3 * k + 2], recv.at[p], at_y(far))
    for d in arrivals:
        source = (z + d) % 8
        await_piece(jnp.where(source % 2 == 0, up, down) * 8 + source)
        await_piece((y + 2) % 4 * 8 + source)

    price(idx, table, e32, w1, w2t, b2, w3, h1, h2, values)
    reduce_values(rank, position, values, span, weight_sum, msg, pnl)

    got_mkt[mkt] = msg[...]
    got_pnl[trade] = pnl[...]
    for k in range(1, 8):
        send(msg, got_mkt.at[mkt], t_send.at[k - 1], r_mkt.at[mkt], {"mkt": (mkt + k) % 8})
    for k in range(1, 8):
        send(pnl, got_pnl.at[trade], t_send.at[6 + k], r_pnl.at[trade], {"trade": (trade + k) % 8})
    for k in range(1, 8):
        other = (mkt + k) % 8
        copy(msg, got_mkt.at[other], t_send.at[0], r_mkt.at[other], {"mkt": other}).wait_recv()
    total = got_mkt[0]
    for k in range(1, 8):
        total = total + got_mkt[k]
    got_marg[scen] = total[:16]
    got_short[part] = total[16:]
    for k in range(1, 32):
        other = (part + k) % 32
        send(
            got_short.at[part], got_short.at[part], t_send.at[16 + k], r_short.at[part],
            {"trade": other // 4, "scen": other % 4},
        )
    for k in range(1, 4):
        send(got_marg.at[scen], got_marg.at[scen], t_send.at[13 + k], r_marg.at[scen], {"scen": (scen + k) % 4})
    for k in range(1, 8):
        other = (trade + k) % 8
        copy(pnl, got_pnl.at[other], t_send.at[0], r_pnl.at[other], {"trade": other}).wait_recv()
    total = got_pnl[0]
    for k in range(1, 8):
        total = total + got_pnl[k]
    pnl_out[...] = total
    for k in range(1, 4):
        other = (scen + k) % 4
        copy(got_marg.at[other], got_marg.at[other], t_send.at[0], r_marg.at[other], {"scen": other}).wait_recv()
    marg_out[...] = (got_marg[0] + got_marg[1]) + (got_marg[2] + got_marg[3])
    for k in range(1, 32):
        other = (part + k) % 32
        copy(
            got_short.at[other], got_short.at[other], t_send.at[0], r_short.at[other], {"scen": scen}
        ).wait_recv()
    total = got_short[0]
    for k in range(1, 32):
        total = total + got_short[k]
    short_out[...] = total
    for c in sends:
        c.wait_send()


def local(quotes, kernel, trade_block, trade_embed, position, scen_rank, w_in, w_mid, b_mid, w_out):
    rows, quote_count = quotes.shape
    blocks = kernel.shape[0]
    scen_total = scen_rank.shape[0] * lax.axis_size("mkt") * lax.axis_size("scen")
    span = scen_total // 20
    weight_sum = math.fsum(math.exp(-r / span) for r in range(scen_total))
    trades, hid = trade_embed.shape
    groups = trades // 16
    slots = 2 * UNROLL
    vmem, smem = pl.BlockSpec(memory_space=pltpu.VMEM), pl.BlockSpec(memory_space=pltpu.SMEM)
    hbm = pl.BlockSpec(memory_space=pl.ANY)
    bf16, f32 = jnp.bfloat16, jnp.float32
    dma = pltpu.SemaphoreType.DMA
    marg, pnl, short = pl.pallas_call(
        functools.partial(fused_kernel, span, weight_sum, quote_count),
        out_shape=(
            jax.ShapeDtypeStruct((16, groups), f32),
            jax.ShapeDtypeStruct((8, 128), f32),
            jax.ShapeDtypeStruct((8, 128), f32),
        ),
        in_specs=[hbm, hbm, hbm, smem, smem] + [vmem] * 5,
        out_specs=(vmem, vmem, vmem),
        scratch_shapes=[
            pltpu.VMEM((rows, SLAB), bf16),
            pltpu.VMEM(kernel.shape, bf16),
            pltpu.VMEM(trade_embed.shape, bf16),
            pltpu.VMEM((rows // 16, blocks, 16, SEG), bf16),
            pltpu.VMEM((32 * blocks, 16, SEG), bf16),
            pltpu.VMEM((2, trades, 128), f32),
            pltpu.VMEM((SEG, hid), bf16),
            pltpu.VMEM((hid, hid), bf16),
            pltpu.VMEM((hid, 256), f32),
            pltpu.VMEM((16, hid), bf16),
            pltpu.VMEM((slots, 256, hid), bf16),
            pltpu.VMEM((slots, hid, 256), bf16),
            pltpu.VMEM((groups, 256), f32),
            pltpu.VMEM((24, groups), f32),
            pltpu.VMEM((8, 128), f32),
            pltpu.VMEM((8, 24, groups), f32),
            pltpu.VMEM((8, 8, 128), f32),
            pltpu.VMEM((4, 16, groups), f32),
            pltpu.VMEM((32, 8, 128), f32),
            dma((3,)), dma((7,)), dma((24,)), dma((32,)), dma((48,)), dma((8,)), dma((8,)), dma((4,)), dma((32,)),
        ],
        compiler_params=pltpu.CompilerParams(
            vmem_limit_bytes=48 << 20, collective_id=0, has_side_effects=True
        ),
        name="shortfall",
    )(
        quotes, kernel, trade_embed, trade_block, scen_rank, position.reshape(16, groups), w_in, w_mid, b_mid, w_out
    )
    return (pnl[0, :16], marg.reshape(-1), short[0, 0])


def solution(mesh):
    placed = (
        P("mkt", None),
        P(("trade", "scen"), None, None),
        P("trade"),
        P("trade", None),
        P("trade"),
        P(("mkt", "scen")),
        P(),
        P(),
        P(),
        P(),
    )
    return jax.shard_map(
        local,
        mesh=mesh,
        in_specs=placed,
        out_specs=(P(("mkt", "scen")), P("trade"), P()),
        check_vma=False,
    )
```

```python
import functools
import math

import jax
import jax.numpy as jnp
from jax import lax
from jax.experimental import pallas as pl
from jax.experimental.pallas import tpu as pltpu
from jax.sharding import PartitionSpec as P

SEG = 128
WIN = 128
QSTEP = 8
SLAB = 384
LAG = 3
ORDER = (1, 7, 2, 6, 4, 3, 5)
HIGHEST = lax.Precision.HIGHEST
MESH = pl.DeviceIdType.MESH
UNROLL = 4


def prepare(w_in, w_mid, b_mid, w_out, embed, e32, w1, w2t, b2, w3):
    w1[...] = (w_in[...].astype(jnp.float32) * 0.5).astype(jnp.bfloat16)
    w2t[...] = (w_mid[...].astype(jnp.float32).T * 0.5).astype(jnp.bfloat16)
    b2[...] = jnp.broadcast_to(b_mid[...].reshape(1, -1) * 0.5, b2.shape[::-1]).T
    w3[...] = jnp.broadcast_to(w_out[...].reshape(1, -1), w3.shape)

    @pl.loop(0, embed.shape[0] // 64)
    def _(i):
        r = pl.multiple_of(i * 64, 64)
        t = embed[pl.ds(r, 64), :].astype(jnp.float32) * 0.5
        e32[0, pl.ds(r, 64), :] = t[:, :128]
        e32[1, pl.ds(r, 64), :] = t[:, 128:]


def price(half, idx, table, e32, w1, w2t, b2, w3, h1, h2, values, beside=lambda k: None):
    groups = values.shape[1] // 2
    u_count = UNROLL
    trades = [(c, j) for c in range(2) for j in range(16)]

    def row(g, c, j):
        return j * 2 * groups + c * groups + g

    def first(g, slot):
        x = jnp.concatenate([table[idx[row(g, c, j)]] for c, j in trades], axis=0).astype(jnp.bfloat16)
        e = jnp.concatenate(
            [
                jnp.concatenate([e32.at[i][pl.ds(row(g, c, j), 8, stride=0), :] for c, j in trades], axis=0)
                for i in range(2)
            ],
            axis=1,
        )
        z = jnp.dot(x, w1[...], preferred_element_type=jnp.float32) + e
        h1[slot] = (z + z * jnp.tanh(z)).astype(jnp.bfloat16)

    def second(slot):
        z = lax.dot_general(w2t[...], h1[slot], (((1,), (1,)), ((), ())), preferred_element_type=jnp.float32)
        z = z + b2[...]
        h2[slot] = (z + z * jnp.tanh(z)).astype(jnp.bfloat16)

    def third(g, slot):
        v = jnp.dot(w3[...], h2[slot], preferred_element_type=jnp.float32)
        values[half, pl.ds(g, 1), :] = v[0:1, :128]
        values[half, pl.ds(g + groups, 1), :] = v[0:1, 128:]

    def step(i, a, b):
        for u in range(u_count):
            first(jnp.minimum((i + 2) * u_count + u, groups - 1), a + u)
            second(b + u)
            third(i * u_count + u, a + u)

    for u in range(u_count):
        first(u, u)
    for u in range(u_count):
        second(u)
        first(u_count + u, u_count + u)

    @pl.loop(0, groups // u_count // 2)
    def _(k):
        beside(k)
        step(2 * k, 0, u_count)
        step(2 * k + 1, u_count, 0)


def prepare_reduce(rank, position, span, weight_sum, picked, spread):
    width = picked.shape[1]
    row = lax.broadcasted_iota(jnp.int32, (16, width), 0)
    lane = lax.broadcasted_iota(jnp.int32, (16, width), 1)
    ranks = jnp.zeros((16, width), jnp.float32)
    for s in range(16):
        ranks = jnp.where(lane // 128 * 8 + lane % 8 == s, rank[s].astype(jnp.float32), ranks)
    weights = jnp.exp(-ranks / span) * (1.0 / weight_sum)
    mine = row == lane % 128 // 8
    picked[0:16] = jnp.where(mine, weights, 0.0)
    picked[16:24] = weights[0:8]
    spread[...] = jnp.dot(
        position[...].T, jnp.where(mine, 1.0, 0.0), precision=HIGHEST, preferred_element_type=jnp.float32
    )


def reduce_values(values, picked, spread, marg, pnl):
    width = picked.shape[1]
    groups = values.shape[1]
    v = jnp.concatenate([values[0], values[1]], axis=1)
    marg[0:16] = -lax.dot_general(
        picked[0:16], v, (((1,), (1,)), ((), ())), precision=HIGHEST, preferred_element_type=jnp.float32
    )
    held = jnp.sum(v * spread[...], axis=0, keepdims=True)
    marg[16:24] = jnp.broadcast_to(-jnp.sum(held * picked[16:17], axis=1, keepdims=True), (8, groups))
    lane = lax.broadcasted_iota(jnp.int32, (width, 128), 0)
    fold = lane // 128 * 8 + lane % 8 == lax.broadcasted_iota(jnp.int32, (width, 128), 1)
    pnl[...] = jnp.dot(
        jnp.broadcast_to(held, (8, width)), jnp.where(fold, 1.0, 0.0),
        precision=HIGHEST, preferred_element_type=jnp.float32,
    )[0:1]


def build(slab, kernel, offset, built):
    for j in range(kernel.shape[0]):
        pick = lax.broadcasted_iota(jnp.int32, (SLAB, WIN), 0) == lax.broadcasted_iota(jnp.int32, (SLAB, WIN), 1) + offset(j)
        window = jnp.dot(
            slab[...], jnp.where(pick, 1.0, 0.0).astype(jnp.bfloat16), preferred_element_type=jnp.float32
        ).astype(jnp.bfloat16)
        state = jnp.dot(window, kernel[j], preferred_element_type=jnp.float32)
        for r in range(slab.shape[0] // 8):
            built[r % 2, r // 2, j] = state[8 * r : 8 * r + 8].astype(jnp.bfloat16)


def fused_kernel(
    span, weight_sum, quote_count,
    quotes_hbm, kernel_hbm, embed_hbm, idx_hbm, rank_hbm, position_hbm, w_in_hbm, w_mid_hbm, b_mid_hbm, w_out_hbm,
    marg_out, pnl_out, short_out,
    slab, kernel, embed, idx, rank, position, w_in, w_mid, b_mid, w_out, spread, picked, built, landed, table, e32, w1, w2t, b2, w3, h1, h2, values, msg, pnl,
    got_mkt, got_pnl, got_marg, got_short, load_sem, z_send, y_send, recv, t_send, r_mkt, r_pnl, r_marg, r_short,
):
    mkt, trade, scen = lax.axis_index("mkt"), lax.axis_index("trade"), lax.axis_index("scen")
    y, z_hi = trade // 2, trade % 2
    z = z_hi * 4 + scen
    part = y * 8 + z
    blocks = kernel.shape[0]

    def at_z(zz):
        return {"trade": y * 2 + zz // 4, "scen": zz % 4}

    def at_y(yy):
        return {"trade": yy * 2 + z_hi}

    base = jnp.clip((part - 1) * 128, 0, quote_count - SLAB)
    loads = [
        pltpu.make_async_copy(quotes_hbm.at[:, pl.ds(pl.multiple_of(base, 128), SLAB)], slab, load_sem.at[0]),
        pltpu.make_async_copy(kernel_hbm, kernel, load_sem.at[1]),
    ] + [
        pltpu.make_async_copy(src, dst, load_sem.at[2 + i])
        for i, (src, dst) in enumerate(
            [
                (embed_hbm, embed), (idx_hbm, idx), (rank_hbm, rank), (position_hbm, position),
                (w_in_hbm, w_in), (w_mid_hbm, w_mid), (b_mid_hbm, b_mid), (w_out_hbm, w_out),
            ]
        )
    ]
    for load in loads:
        load.start()

    barrier = pltpu.get_barrier_semaphore()
    up, down = (y + 1) % 4, (y + 3) % 4
    for k in range(1, 8):
        pl.semaphore_signal(barrier, inc=1, device_id=at_z((z + k) % 8), device_id_type=MESH)
        pl.semaphore_signal(barrier, inc=1, device_id={"mkt": (mkt + k) % 8}, device_id_type=MESH)
    pl.semaphore_signal(barrier, inc=1, device_id=at_y(up), device_id_type=MESH)
    pl.semaphore_signal(barrier, inc=1, device_id=at_y(down), device_id_type=MESH)

    def offset(j):
        return jnp.clip(QSTEP * (part * blocks + j) - (WIN - QSTEP) // 2, 0, quote_count - WIN) - base

    loads[0].wait()
    loads[1].wait()
    build(slab, kernel, offset, built)
    for h in range(2):
        landed[h, pl.ds(part * blocks, blocks)] = built[h, scen]
    pl.semaphore_wait(barrier, 16)

    def copy(src, dst, send, receive, device):
        return pltpu.make_async_remote_copy(
            src_ref=src, dst_ref=dst, send_sem=send, recv_sem=receive, device_id=device, device_id_type=MESH
        )

    sends = []

    def send(*args):
        c = copy(*args)
        c.start()
        sends.append(c)

    def piece(h, p):
        return landed.at[h, pl.ds(p * blocks, blocks)]

    def widen(h, p):
        at = pl.ds(p * blocks, blocks)
        table[h, at] = landed[h, at].astype(jnp.float32)

    def await_piece(h, p):
        copy(piece(h, p), piece(h, p), y_send.at[h, 0], recv.at[h, p], at_y(up)).wait_recv()
        widen(h, p)

    def arrival(k):
        return (z + 8 - (0, *ORDER)[k]) % 8

    def first_hop(h, k, start=True):
        p = y * 8 + arrival(k)
        hops = [
            copy(piece(h, p), piece(h, p), y_send.at[h, 3 * k + i], recv.at[h, p], at_y(to))
            for i, to in enumerate((up, down))
        ]
        for hop in hops:
            if start:
                hop.start()
            else:
                hop.wait_send()

    def second_hop(h, k, start=True):
        source = arrival(k)
        even = source % 2 == 0
        near, far = jnp.where(even, down, up), jnp.where(even, up, down)
        p = near * 8 + source
        hop = copy(piece(h, p), piece(h, p), y_send.at[h, 3 * k + 2], recv.at[h, p], at_y(far))
        if start:
            await_piece(h, p)
            hop.start()
        else:
            hop.wait_send()

    def rest(h, k):
        source = arrival(k)
        await_piece(h, jnp.where(source % 2 == 0, up, down) * 8 + source)
        await_piece(h, (y + 2) % 4 * 8 + source)

    for h in range(2):
        for k, d in enumerate(ORDER):
            to = (z + d) % 8
            send(built.at[h, to % 4], piece(h, part), z_send.at[h, k], recv.at[h, part], at_z(to))

    for k in range(8):
        if k:
            await_piece(0, y * 8 + arrival(k))
        first_hop(0, k)
        if k == 0:
            widen(0, part)
            widen(1, part)
            for load in loads[2:]:
                load.wait()
            prepare(w_in, w_mid, b_mid, w_out, embed, e32, w1, w2t, b2, w3)
            prepare_reduce(rank, position, span, weight_sum, picked, spread)
        if k >= LAG:
            second_hop(0, k - LAG)
    for k in range(8 - LAG, 8):
        second_hop(0, k)
    for k in range(8):
        if k:
            await_piece(1, y * 8 + arrival(k))
        first_hop(1, k)
    for k in range(8):
        rest(0, k)

    def beside(step):
        for pair in range(4):
            @pl.when(step == pair)
            def _():
                second_hop(1, 2 * pair)
                second_hop(1, 2 * pair + 1)

    price(0, idx, table.at[0], e32, w1, w2t, b2, w3, h1, h2, values, beside)
    for k in range(8):
        rest(1, k)
    price(1, idx, table.at[1], e32, w1, w2t, b2, w3, h1, h2, values)
    reduce_values(values, picked, spread, msg, pnl)

    got_mkt[mkt] = msg[...]
    got_pnl[trade] = pnl[...]
    for k in range(1, 8):
        send(msg, got_mkt.at[mkt], t_send.at[k - 1], r_mkt.at[mkt], {"mkt": (mkt + k) % 8})
    for k in range(1, 8):
        send(pnl, got_pnl.at[trade], t_send.at[6 + k], r_pnl.at[trade], {"trade": (trade + k) % 8})
    for k in range(1, 8):
        other = (mkt + k) % 8
        copy(msg, got_mkt.at[other], t_send.at[0], r_mkt.at[other], {"mkt": other}).wait_recv()
    total = got_mkt[0]
    for k in range(1, 8):
        total = total + got_mkt[k]
    got_marg[scen] = total[:16]
    got_short[part] = total[16:17]
    for k in range(1, 32):
        other = (part + k) % 32
        send(
            got_short.at[part], got_short.at[part], t_send.at[16 + k], r_short.at[part],
            {"trade": other // 4, "scen": other % 4},
        )
    for k in range(1, 4):
        send(got_marg.at[scen], got_marg.at[scen], t_send.at[13 + k], r_marg.at[scen], {"scen": (scen + k) % 4})
    for k in range(1, 8):
        other = (trade + k) % 8
        copy(pnl, got_pnl.at[other], t_send.at[0], r_pnl.at[other], {"trade": other}).wait_recv()
    total = got_pnl[0]
    for k in range(1, 8):
        total = total + got_pnl[k]
    pnl_out[...] = total[0, :16]
    for k in range(1, 4):
        other = (scen + k) % 4
        copy(got_marg.at[other], got_marg.at[other], t_send.at[0], r_marg.at[other], {"scen": other}).wait_recv()
    marg_out[...] = ((got_marg[0] + got_marg[1]) + (got_marg[2] + got_marg[3])).reshape(-1)
    for k in range(1, 32):
        other = (part + k) % 32
        copy(
            got_short.at[other], got_short.at[other], t_send.at[0], r_short.at[other], {"scen": scen}
        ).wait_recv()
    total = got_short[0]
    for k in range(1, 32):
        total = total + got_short[k]
    short_out[...] = total[0, :1]
    for c in sends:
        c.wait_send()
    for h in range(2):
        for k in range(8):
            first_hop(h, k, start=False)
            second_hop(h, k, start=False)


def local(quotes, kernel, trade_block, trade_embed, position, scen_rank, w_in, w_mid, b_mid, w_out):
    rows, quote_count = quotes.shape
    blocks = kernel.shape[0]
    scen_total = scen_rank.shape[0] * lax.axis_size("mkt") * lax.axis_size("scen")
    span = scen_total // 20
    weight_sum = math.fsum(math.exp(-r / span) for r in range(scen_total))
    trades, hid = trade_embed.shape
    groups = trades // 16
    slots = 2 * UNROLL
    vmem = pl.BlockSpec(memory_space=pltpu.VMEM)
    hbm = pl.BlockSpec(memory_space=pl.ANY)
    bf16, f32 = jnp.bfloat16, jnp.float32
    dma = pltpu.SemaphoreType.DMA
    marg, pnl, short = pl.pallas_call(
        functools.partial(fused_kernel, span, weight_sum, quote_count),
        out_shape=(
            jax.ShapeDtypeStruct((trades,), f32),
            jax.ShapeDtypeStruct((16,), f32),
            jax.ShapeDtypeStruct((1,), f32),
        ),
        in_specs=[hbm] * 10,
        out_specs=(vmem, vmem, vmem),
        scratch_shapes=[
            pltpu.VMEM((rows, SLAB), bf16),
            pltpu.VMEM(kernel.shape, bf16),
            pltpu.VMEM(trade_embed.shape, bf16),
            pltpu.SMEM(trade_block.shape, jnp.int32),
            pltpu.SMEM(scen_rank.shape, jnp.int32),
            pltpu.VMEM((16, groups), f32),
            pltpu.VMEM(w_in.shape, bf16),
            pltpu.VMEM(w_mid.shape, bf16),
            pltpu.VMEM(b_mid.shape, f32),
            pltpu.VMEM(w_out.shape, bf16),
            pltpu.VMEM((groups, 256), f32),
            pltpu.VMEM((24, 256), f32),
            pltpu.VMEM((2, rows // 16, blocks, 8, SEG), bf16),
            pltpu.VMEM((2, 32 * blocks, 8, SEG), bf16),
            pltpu.VMEM((2, 32 * blocks, 8, SEG), f32),
            pltpu.VMEM((2, trades, 128), f32),
            pltpu.VMEM((SEG, hid), bf16),
            pltpu.VMEM((hid, hid), bf16),
            pltpu.VMEM((hid, 256), f32),
            pltpu.VMEM((16, hid), bf16),
            pltpu.VMEM((slots, 256, hid), bf16),
            pltpu.VMEM((slots, hid, 256), bf16),
            pltpu.VMEM((2, groups, 128), f32),
            pltpu.VMEM((24, groups), f32),
            pltpu.VMEM((1, 128), f32),
            pltpu.VMEM((8, 24, groups), f32),
            pltpu.VMEM((8, 1, 128), f32),
            pltpu.VMEM((4, 16, groups), f32),
            pltpu.VMEM((32, 1, 128), f32),
            dma((10,)), dma((2, 7)), dma((2, 24)), dma((2, 32)), dma((48,)), dma((8,)), dma((8,)), dma((4,)), dma((32,)),
        ],
        compiler_params=pltpu.CompilerParams(
            vmem_limit_bytes=40 << 20, collective_id=0, has_side_effects=True
        ),
        name="shortfall",
    )(
        *(
            pltpu.with_memory_space_constraint(a, pltpu.HBM)
            for a in (
                quotes, kernel, trade_embed, trade_block, scen_rank, position.reshape(16, groups),
                w_in, w_mid, b_mid, w_out,
            )
        )
    )
    return (pnl, marg, short[0])


def solution(mesh):
    placed = (
        P("mkt", None),
        P(("trade", "scen"), None, None),
        P("trade"),
        P("trade", None),
        P("trade"),
        P(("mkt", "scen")),
        P(),
        P(),
        P(),
        P(),
    )
    return jax.shard_map(
        local,
        mesh=mesh,
        in_specs=placed,
        out_specs=(P(("mkt", "scen")), P("trade"), P()),
        check_vma=False,
    )
```

```python
import functools
import math

import jax
import jax.numpy as jnp
from jax import lax
from jax.experimental import pallas as pl
from jax.experimental.pallas import tpu as pltpu
from jax.sharding import PartitionSpec as P

SEG = 128
WIN = 128
QSTEP = 8
SLAB = 384
ORDER = (1, 7, 2, 6, 4, 3, 5)
DIRECT = frozenset([(0, 0), (0, 1), (0, 2), (0, 3), (0, 4), (0, 5), (0, 6), (0, 7), (1, 0), (1, 1), (1, 2), (1, 3), (1, 4), (1, 5), (1, 6), (1, 7)])
EXCHANGE = (
    (0, 1, 0),
    (0, 1, 1),
    (0, 1, 2),
    (0, 1, 3),
    (0, 1, 4),
    (0, 1, 5),
    (0, 1, 6),
    (0, 1, 7),
    (1, 1, 0),
    (1, 1, 1),
    (1, 1, 2),
    (1, 1, 3),
    (1, 1, 4),
    (1, 1, 5),
    (1, 1, 6),
    (1, 1, 7),
)
LATER = ()
HIGHEST = lax.Precision.HIGHEST
MESH = pl.DeviceIdType.MESH
UNROLL = 4


def prepare(w_in, w_mid, b_mid, w_out, embed, e32, w1, w2t, b2, w3):
    w1[...] = (w_in[...].astype(jnp.float32) * 0.5).astype(jnp.bfloat16)
    w2t[...] = (w_mid[...].astype(jnp.float32).T * 0.5).astype(jnp.bfloat16)
    b2[...] = jnp.broadcast_to(b_mid[...].reshape(1, -1) * 0.5, b2.shape[::-1]).T
    w3[...] = jnp.broadcast_to(w_out[...].reshape(1, -1), w3.shape)

    @pl.loop(0, embed.shape[0] // 64)
    def _(i):
        r = pl.multiple_of(i * 64, 64)
        t = embed[pl.ds(r, 64), :].astype(jnp.float32) * 0.5
        e32[0, pl.ds(r, 64), :] = t[:, :128]
        e32[1, pl.ds(r, 64), :] = t[:, 128:]


def price(idx, table, e32, w1, w2t, b2, w3, h1, h2, values, beside, between):
    groups = values.shape[1] // 2
    u_count = UNROLL
    trades = [(c, j) for c in range(2) for j in range(16)]
    chunks = groups // u_count

    def row(g, c, j):
        return j * 2 * groups + c * groups + g

    def first(half, g, slot):
        x = jnp.concatenate([table[half, idx[row(g, c, j)]] for c, j in trades], axis=0).astype(jnp.bfloat16)
        e = jnp.concatenate(
            [
                jnp.concatenate([e32.at[i][pl.ds(row(g, c, j), 8, stride=0), :] for c, j in trades], axis=0)
                for i in range(2)
            ],
            axis=1,
        )
        z = jnp.dot(x, w1[...], preferred_element_type=jnp.float32) + e
        h1[slot] = (z + z * jnp.tanh(z)).astype(jnp.bfloat16)

    def second(slot):
        z = lax.dot_general(w2t[...], h1[slot], (((1,), (1,)), ((), ())), preferred_element_type=jnp.float32)
        z = z + b2[...]
        h2[slot] = (z + z * jnp.tanh(z)).astype(jnp.bfloat16)

    def third(half, g, slot):
        v = jnp.dot(w3[...], h2[slot], preferred_element_type=jnp.float32)
        values[half, pl.ds(g, 1), :] = v[0:1, :128]
        values[half, pl.ds(g + groups, 1), :] = v[0:1, 128:]

    def step(parity, last, middle, ahead):
        a, b = parity * u_count, (1 - parity) * u_count
        for u in range(u_count):
            if ahead is not None:
                first(ahead[0], ahead[1] * u_count + u, a + u)
            if middle:
                second(b + u)
            third(last[0], last[1] * u_count + u, a + u)

    for u in range(u_count):
        first(0, u, u)
    for u in range(u_count):
        second(u)
        first(0, u_count + u, u_count + u)

    for half in range(2):
        @pl.loop(0, chunks // 2 - 1)
        def _(k):
            if half == 0:
                beside(k)
            step(0, (half, 2 * k), True, (half, 2 * k + 2))
            step(1, (half, 2 * k + 1), True, (half, 2 * k + 3))

        if half == 0:
            between()
        ahead = ((1, 0), (1, 1)) if half == 0 else (None, None)
        step(0, (half, chunks - 2), True, ahead[0])
        step(1, (half, chunks - 1), half == 0, ahead[1])


def prepare_reduce(rank, position, span, weight_sum, picked, spread):
    width = picked.shape[1]
    row = lax.broadcasted_iota(jnp.int32, (16, width), 0)
    lane = lax.broadcasted_iota(jnp.int32, (16, width), 1)
    ranks = jnp.zeros((16, width), jnp.float32)
    for s in range(16):
        ranks = jnp.where(lane // 128 * 8 + lane % 8 == s, rank[s].astype(jnp.float32), ranks)
    weights = jnp.exp(-ranks / span) * (1.0 / weight_sum)
    mine = row == lane % 128 // 8
    picked[0:16] = jnp.where(mine, weights, 0.0)
    picked[16:24] = weights[0:8]
    spread[...] = jnp.dot(
        position[...].T, jnp.where(mine, 1.0, 0.0), precision=HIGHEST, preferred_element_type=jnp.float32
    )


def reduce_trades(values, picked, spread, pnl, short):
    width = picked.shape[1]
    held = jnp.concatenate(
        [jnp.sum(values[h] * spread[:, 128 * h : 128 * h + 128], axis=0, keepdims=True) for h in range(2)], axis=1
    )
    short[...] = jnp.broadcast_to(-jnp.sum(held * picked[16:17], axis=1, keepdims=True), short.shape)
    lane = lax.broadcasted_iota(jnp.int32, (width, 128), 0)
    fold = lane // 128 * 8 + lane % 8 == lax.broadcasted_iota(jnp.int32, (width, 128), 1)
    pnl[...] = jnp.dot(
        jnp.broadcast_to(held, (8, width)), jnp.where(fold, 1.0, 0.0),
        precision=HIGHEST, preferred_element_type=jnp.float32,
    )[0:1]


def reduce_scenarios(values, picked, marg):
    v = jnp.concatenate([values[0], values[1]], axis=1)
    marg[...] = -lax.dot_general(
        picked[0:16], v, (((1,), (1,)), ((), ())), precision=HIGHEST, preferred_element_type=jnp.float32
    )


def select(offset, picks):
    apart = lax.broadcasted_iota(jnp.int32, (SLAB, WIN), 0) - lax.broadcasted_iota(jnp.int32, (SLAB, WIN), 1)
    for j in range(picks.shape[0]):
        picks[j] = jnp.where(apart == offset(j), 1.0, 0.0).astype(jnp.bfloat16)


def build(slab, kernel, picks, built):
    for j in range(kernel.shape[0]):
        window = jnp.dot(slab[...], picks[j], preferred_element_type=jnp.float32).astype(jnp.bfloat16)
        state = jnp.dot(window, kernel[j], preferred_element_type=jnp.float32)
        for r in range(slab.shape[0] // 8):
            built[r % 2, r // 2, j] = state[8 * r : 8 * r + 8].astype(jnp.bfloat16)


def fused_kernel(
    span, weight_sum, quote_count,
    quotes_hbm, kernel_hbm, embed_hbm, idx_hbm, rank_hbm, position_hbm, w_in_hbm, w_mid_hbm, b_mid_hbm, w_out_hbm,
    marg_out, pnl_out, short_out,
    slab, picks, kernel, embed, idx, rank, position, w_in, w_mid, b_mid, w_out, spread, picked, built, landed, table, e32, w1, w2t, b2, w3, h1, h2, values, msg, pnl, short,
    got_mkt, got_sum, got_pnl, got_marg, got_short, load_sem, z_send, y_send, recv, t_send, r_mkt, r_sum, r_pnl, r_marg, r_short,
):
    mkt, trade, scen = lax.axis_index("mkt"), lax.axis_index("trade"), lax.axis_index("scen")
    y, z_hi = trade // 2, trade % 2
    z = z_hi * 4 + scen
    part = y * 8 + z
    blocks = kernel.shape[0]

    def at_z(zz):
        return {"trade": y * 2 + zz // 4, "scen": zz % 4}

    def at_y(yy):
        return {"trade": yy * 2 + z_hi}

    base = jnp.clip((part - 1) * 128, 0, quote_count - SLAB)
    loads = [
        pltpu.make_async_copy(quotes_hbm.at[:, pl.ds(pl.multiple_of(base, 128), SLAB)], slab, load_sem.at[0]),
        pltpu.make_async_copy(kernel_hbm, kernel, load_sem.at[1]),
    ] + [
        pltpu.make_async_copy(src, dst, load_sem.at[2 + i])
        for i, (src, dst) in enumerate(
            [
                (embed_hbm, embed), (idx_hbm, idx), (rank_hbm, rank), (position_hbm, position),
                (w_in_hbm, w_in), (w_mid_hbm, w_mid), (b_mid_hbm, b_mid), (w_out_hbm, w_out),
            ]
        )
    ]
    for load in loads:
        load.start()

    barrier = pltpu.get_barrier_semaphore()
    up, down = (y + 1) % 4, (y + 3) % 4
    for k in range(1, 8):
        pl.semaphore_signal(barrier, inc=1, device_id=at_z((z + k) % 8), device_id_type=MESH)
        pl.semaphore_signal(barrier, inc=1, device_id={"mkt": (mkt + k) % 8}, device_id_type=MESH)
    for k in range(1, 4):
        pl.semaphore_signal(barrier, inc=1, device_id=at_y((y + k) % 4), device_id_type=MESH)

    def offset(j):
        return jnp.clip(QSTEP * (part * blocks + j) - (WIN - QSTEP) // 2, 0, quote_count - WIN) - base

    select(offset, picks)
    loads[0].wait()
    loads[1].wait()
    build(slab, kernel, picks, built)
    for h in range(2):
        landed[h, pl.ds(part * blocks, blocks)] = built[h, scen]
    pl.semaphore_wait(barrier, 17)

    def copy(src, dst, send, receive, device):
        return pltpu.make_async_remote_copy(
            src_ref=src, dst_ref=dst, send_sem=send, recv_sem=receive, device_id=device, device_id_type=MESH
        )

    sends = []

    def send(*args):
        c = copy(*args)
        c.start()
        sends.append(c)

    def piece(h, p):
        return landed.at[h, pl.ds(p * blocks, blocks)]

    def widen(h, p):
        at = pl.ds(p * blocks, blocks)
        table[h, at] = landed[h, at].astype(jnp.float32)

    def await_piece(h, p):
        copy(piece(h, p), piece(h, p), y_send.at[h, 0], recv.at[h, p], at_y(up)).wait_recv()
        widen(h, p)

    def arrival(k):
        return (z + 8 - (0, *ORDER)[k]) % 8

    def first_hop(h, k, start=True):
        p = y * 8 + arrival(k)
        hops = [
            copy(piece(h, p), piece(h, p), y_send.at[h, 3 * k + i], recv.at[h, p], at_y(to))
            for i, to in enumerate((up, down, (y + 2) % 4) if (h, k) in DIRECT else (up, down))
        ]
        for hop in hops:
            if start:
                hop.start()
            else:
                hop.wait_send()

    def second_hop(h, k, start=True):
        if (h, k) in DIRECT:
            return
        source = arrival(k)
        even = source % 2 == 0
        near, far = jnp.where(even, down, up), jnp.where(even, up, down)
        p = near * 8 + source
        hop = copy(piece(h, p), piece(h, p), y_send.at[h, 3 * k + 2], recv.at[h, p], at_y(far))
        if start:
            await_piece(h, p)
            hop.start()
        else:
            hop.wait_send()

    def rest(h, k):
        source = arrival(k)
        await_piece(h, jnp.where(source % 2 == 0, up, down) * 8 + source)
        if (h, k) in DIRECT:
            await_piece(h, jnp.where(source % 2 == 0, down, up) * 8 + source)
        await_piece(h, (y + 2) % 4 * 8 + source)

    for h in range(2):
        for k, d in enumerate(ORDER):
            to = (z + d) % 8
            send(built.at[h, to % 4], piece(h, part), z_send.at[h, k], recv.at[h, part], at_z(to))

    widen(0, part)
    widen(1, part)
    for h, hop, k in EXCHANGE:
        if hop == 2:
            second_hop(h, k)
        else:
            if k:
                await_piece(h, y * 8 + arrival(k))
            first_hop(h, k)
            if h == 0 and k == 0:
                for load in loads[2:]:
                    load.wait()
                prepare(w_in, w_mid, b_mid, w_out, embed, e32, w1, w2t, b2, w3)
                prepare_reduce(rank, position, span, weight_sum, picked, spread)
    for k in range(8):
        rest(0, k)

    def beside(step):
        for at, hops in enumerate(LATER):
            @pl.when(step == at)
            def _():
                for k in hops:
                    second_hop(1, k)

    def between():
        for k in range(8):
            rest(1, k)

    price(idx, table, e32, w1, w2t, b2, w3, h1, h2, values, beside, between)
    reduce_trades(values, picked, spread, pnl, short)
    got_sum[mkt] = short[...]
    got_pnl[trade] = pnl[...]
    for k in range(1, 8):
        send(short, got_sum.at[mkt], t_send.at[47 + k], r_sum.at[mkt], {"mkt": (mkt + k) % 8})
    for k in range(1, 8):
        send(pnl, got_pnl.at[trade], t_send.at[6 + k], r_pnl.at[trade], {"trade": (trade + k) % 8})
    reduce_scenarios(values, picked, msg)
    got_mkt[mkt] = msg[...]
    for k in range(1, 8):
        send(msg, got_mkt.at[mkt], t_send.at[k - 1], r_mkt.at[mkt], {"mkt": (mkt + k) % 8})
    for k in range(1, 8):
        other = (mkt + k) % 8
        copy(short, got_sum.at[other], t_send.at[0], r_sum.at[other], {"mkt": other}).wait_recv()
    total = got_sum[0]
    for k in range(1, 8):
        total = total + got_sum[k]
    got_short[part] = total
    for k in range(1, 32):
        other = (part + k) % 32
        send(
            got_short.at[part], got_short.at[part], t_send.at[16 + k], r_short.at[part],
            {"trade": other // 4, "scen": other % 4},
        )
    for k in range(1, 8):
        other = (mkt + k) % 8
        copy(msg, got_mkt.at[other], t_send.at[0], r_mkt.at[other], {"mkt": other}).wait_recv()
    total = got_mkt[0]
    for k in range(1, 8):
        total = total + got_mkt[k]
    got_marg[scen] = total
    for k in range(1, 4):
        send(got_marg.at[scen], got_marg.at[scen], t_send.at[13 + k], r_marg.at[scen], {"scen": (scen + k) % 4})
    for k in range(1, 8):
        other = (trade + k) % 8
        copy(pnl, got_pnl.at[other], t_send.at[0], r_pnl.at[other], {"trade": other}).wait_recv()
    total = got_pnl[0]
    for k in range(1, 8):
        total = total + got_pnl[k]
    pnl_out[...] = total[0, :16]
    for k in range(1, 4):
        other = (scen + k) % 4
        copy(got_marg.at[other], got_marg.at[other], t_send.at[0], r_marg.at[other], {"scen": other}).wait_recv()
    marg_out[...] = ((got_marg[0] + got_marg[1]) + (got_marg[2] + got_marg[3])).reshape(-1)
    for k in range(1, 32):
        other = (part + k) % 32
        copy(
            got_short.at[other], got_short.at[other], t_send.at[0], r_short.at[other], {"scen": scen}
        ).wait_recv()
    total = got_short[0]
    for k in range(1, 32):
        total = total + got_short[k]
    short_out[...] = total[0, :1]
    for c in sends:
        c.wait_send()
    for h in range(2):
        for k in range(8):
            first_hop(h, k, start=False)
            second_hop(h, k, start=False)


def hand_on(marg, pnl, short, marg_out, pnl_out, short_out):
    marg_out[...] = marg[...]
    pnl_out[...] = pnl[...]
    short_out[...] = short[...]


def local(quotes, kernel, trade_block, trade_embed, position, scen_rank, w_in, w_mid, b_mid, w_out):
    rows, quote_count = quotes.shape
    blocks = kernel.shape[0]
    scen_total = scen_rank.shape[0] * lax.axis_size("mkt") * lax.axis_size("scen")
    span = scen_total // 20
    weight_sum = math.fsum(math.exp(-r / span) for r in range(scen_total))
    trades, hid = trade_embed.shape
    groups = trades // 16
    slots = 2 * UNROLL
    vmem = pl.BlockSpec(memory_space=pltpu.VMEM)
    hbm = pl.BlockSpec(memory_space=pl.ANY)
    bf16, f32 = jnp.bfloat16, jnp.float32
    dma = pltpu.SemaphoreType.DMA
    marg, pnl, short = pl.pallas_call(
        functools.partial(fused_kernel, span, weight_sum, quote_count),
        out_shape=(
            jax.ShapeDtypeStruct((trades,), f32),
            jax.ShapeDtypeStruct((16,), f32),
            jax.ShapeDtypeStruct((1,), f32),
        ),
        in_specs=[hbm] * 10,
        out_specs=(vmem, vmem, vmem),
        scratch_shapes=[
            pltpu.VMEM((rows, SLAB), bf16),
            pltpu.VMEM((blocks, SLAB, WIN), bf16),
            pltpu.VMEM(kernel.shape, bf16),
            pltpu.VMEM(trade_embed.shape, bf16),
            pltpu.SMEM(trade_block.shape, jnp.int32),
            pltpu.SMEM(scen_rank.shape, jnp.int32),
            pltpu.VMEM((16, groups), f32),
            pltpu.VMEM(w_in.shape, bf16),
            pltpu.VMEM(w_mid.shape, bf16),
            pltpu.VMEM(b_mid.shape, f32),
            pltpu.VMEM(w_out.shape, bf16),
            pltpu.VMEM((groups, 256), f32),
            pltpu.VMEM((24, 256), f32),
            pltpu.VMEM((2, rows // 16, blocks, 8, SEG), bf16),
            pltpu.VMEM((2, 32 * blocks, 8, SEG), bf16),
            pltpu.VMEM((2, 32 * blocks, 8, SEG), f32),
            pltpu.VMEM((2, trades, 128), f32),
            pltpu.VMEM((SEG, hid), bf16),
            pltpu.VMEM((hid, hid), bf16),
            pltpu.VMEM((hid, 256), f32),
            pltpu.VMEM((16, hid), bf16),
            pltpu.VMEM((slots, 256, hid), bf16),
            pltpu.VMEM((slots, hid, 256), bf16),
            pltpu.VMEM((2, groups, 128), f32),
            pltpu.VMEM((16, groups), f32),
            pltpu.VMEM((1, 128), f32),
            pltpu.VMEM((1, 128), f32),
            pltpu.VMEM((8, 16, groups), f32),
            pltpu.VMEM((8, 1, 128), f32),
            pltpu.VMEM((8, 1, 128), f32),
            pltpu.VMEM((4, 16, groups), f32),
            pltpu.VMEM((32, 1, 128), f32),
            dma((10,)), dma((2, 7)), dma((2, 24)), dma((2, 32)), dma((56,)), dma((8,)), dma((8,)), dma((8,)), dma((4,)), dma((32,)),
        ],
        compiler_params=pltpu.CompilerParams(
            vmem_limit_bytes=40 << 20, collective_id=0, has_side_effects=True
        ),
        name="shortfall",
    )(
        *(
            pltpu.with_memory_space_constraint(a, pltpu.HBM)
            for a in (
                quotes, kernel, trade_embed, trade_block, scen_rank, position.reshape(16, groups),
                w_in, w_mid, b_mid, w_out,
            )
        )
    )
    marg, pnl, short = pl.pallas_call(
        hand_on,
        out_shape=tuple(jax.ShapeDtypeStruct(a.shape, f32) for a in (marg, pnl, short)),
        in_specs=[vmem] * 3,
        out_specs=(vmem,) * 3,
        compiler_params=pltpu.CompilerParams(vmem_limit_bytes=1 << 20),
        name="results",
    )(marg, pnl, short)
    return (pnl, marg, short[0])


def solution(mesh):
    placed = (
        P("mkt", None),
        P(("trade", "scen"), None, None),
        P("trade"),
        P("trade", None),
        P("trade"),
        P(("mkt", "scen")),
        P(),
        P(),
        P(),
        P(),
    )
    return jax.shard_map(
        local,
        mesh=mesh,
        in_specs=placed,
        out_specs=(P(("mkt", "scen")), P("trade"), P()),
        check_vma=False,
    )
```
